16 devices in a mesh: pp: 2 (over z), dp: 8 (over y, x, core).
Axes of the slice: x: 2, y: 2, z: 2, core: 2. Of those that a mesh axis runs over, the one named last changes fastest.
Arguments:
- x_in: bfloat16 [12, 48, 128, 768], P(None, 'dp')
- grad_y: bfloat16 [12, 48, 128, 768], P(None, 'dp')
- w_qkv: bfloat16 [2, 1, 768, 2304], P('pp')
- w_out: bfloat16 [2, 1, 768, 768], P('pp')
- w_up: bfloat16 [2, 1, 768, 3072], P('pp')
- w_down: bfloat16 [2, 1, 3072, 768], P('pp')
Outputs:
- output 1: float32 [2, 1, 768, 2304], P('pp', None, 'dp')
- output 2: float32 [2, 1, 768, 768], P('pp', None, 'dp')
- output 3: float32 [2, 1, 768, 3072], P('pp', None, 'dp')
- output 4: float32 [2, 1, 3072, 768], P('pp', None, 'dp')
- output 5: bfloat16 [12, 48, 128, 768], P(None, 'dp')
All inputs are finite; a program needn't handle non-finite values.
Results may differ from the reference program's by a relative error of at most 0.0188847.
Values are sent between devices in bfloat16 or wider.
A program may use at most 1 GiB of HBM per device.

```python
import jax
import jax.numpy as jnp
from jax import lax

MICROBATCHES = 12
BATCH_DEV = 6
SEQ_LEN = 128
D_MODEL = 768
N_HEADS = 12
LAYERS = 1
STAGES = 2
REPLICAS = 8
HEAD_DIM = D_MODEL // N_HEADS
NORM_EPS = 1e-6


def setup_inputs(seed: int = 0) -> dict:
    key_list = jax.random.split(jax.random.key(seed), 6)
    act_shape = (MICROBATCHES, REPLICAS * BATCH_DEV, SEQ_LEN, D_MODEL)
    stack_dims = (STAGES, LAYERS)
    depth_scale = (STAGES * LAYERS) ** -0.5
    x_in = jax.random.normal(key_list[0], act_shape, jnp.float32)
    grad_y = jax.random.normal(key_list[1], act_shape, jnp.float32)
    w_qkv = jax.random.normal(key_list[2], stack_dims + (D_MODEL, 3 * D_MODEL), jnp.float32) * D_MODEL ** -0.5
    w_out = jax.random.normal(key_list[3], stack_dims + (D_MODEL, D_MODEL), jnp.float32) * (depth_scale * D_MODEL ** -0.5)
    w_up = jax.random.normal(key_list[4], stack_dims + (D_MODEL, 4 * D_MODEL), jnp.float32) * D_MODEL ** -0.5
    w_down = jax.random.normal(key_list[5], stack_dims + (4 * D_MODEL, D_MODEL), jnp.float32) * (depth_scale * (4 * D_MODEL) ** -0.5)
    return {"x_in": x_in.astype(jnp.bfloat16), "grad_y": grad_y.astype(jnp.bfloat16), "w_qkv": w_qkv.astype(jnp.bfloat16), "w_out": w_out.astype(jnp.bfloat16), "w_up": w_up.astype(jnp.bfloat16), "w_down": w_down.astype(jnp.bfloat16)}


def to_bf16(value_in):
    return value_in.astype(jnp.bfloat16).astype(jnp.float32)


def rms_wide(hidden):
    return hidden * lax.rsqrt(jnp.mean(hidden * hidden, axis=-1, keepdims=True) + NORM_EPS)


def layer_apply(hidden, layer_w):
    w_qkv, w_out, w_up, w_down = layer_w
    normed = to_bf16(rms_wide(hidden))
    qkv_act = to_bf16(jnp.einsum("bsd,de->bse", normed, w_qkv))
    qkv_heads = qkv_act.reshape(BATCH_DEV, SEQ_LEN, 3, N_HEADS, HEAD_DIM)
    scores = jnp.einsum("bqhe,bkhe->bhqk", qkv_heads[:, :, 0], qkv_heads[:, :, 1]) * HEAD_DIM ** -0.5
    causal = jnp.arange(SEQ_LEN)[:, None] >= jnp.arange(SEQ_LEN)[None, :]
    attn_probs = to_bf16(jax.nn.softmax(jnp.where(causal, scores, -1e30), axis=-1))
    attn_cat = to_bf16(jnp.einsum("bhqk,bkhe->bqhe", attn_probs, qkv_heads[:, :, 2])).reshape(BATCH_DEV, SEQ_LEN, D_MODEL)
    resid_mid = to_bf16(hidden + jnp.einsum("bsd,de->bse", attn_cat, w_out))
    normed_mid = to_bf16(rms_wide(resid_mid))
    up_act = to_bf16(jnp.einsum("bsd,df->bsf", normed_mid, w_up))
    gelu_act = to_bf16(jax.nn.gelu(up_act, approximate=True))
    return to_bf16(resid_mid + jnp.einsum("bsf,fd->bsd", gelu_act, w_down))


layer_ckpt = jax.checkpoint(layer_apply)


def stack_apply(all_w, hidden):
    def body_fn(hid_state, layer_w):
        return layer_ckpt(hid_state, layer_w), None
    hid_final, _ = lax.scan(body_fn, hidden, all_w)
    return hid_final


def reference(x_in, grad_y, w_qkv, w_out, w_up, w_down):
    n_layers = STAGES * LAYERS
    all_w = tuple(weight.astype(jnp.float32).reshape((n_layers,) + weight.shape[2:]) for weight in (w_qkv, w_out, w_up, w_down))
    rows_x = x_in.reshape(MICROBATCHES * REPLICAS, BATCH_DEV, SEQ_LEN, D_MODEL)
    rows_g = grad_y.reshape(MICROBATCHES * REPLICAS, BATCH_DEV, SEQ_LEN, D_MODEL)

    def micro_step(grad_accs, pair_in):
        hid_in = pair_in[0].astype(jnp.float32)
        y_mb, pull_fn = jax.vjp(lambda weights: stack_apply(weights, hid_in), all_w)
        w_grads = pull_fn(pair_in[1].astype(jnp.float32))[0]
        new_accs = tuple(acc_part + new_part for acc_part, new_part in zip(grad_accs, w_grads))
        return new_accs, y_mb.astype(jnp.bfloat16)

    init_accs = tuple(jnp.zeros(weight.shape, jnp.float32) for weight in all_w)
    grad_accs, y_rows = lax.scan(micro_step, init_accs, (rows_x, rows_g))
    dw_list = [acc_part.reshape((STAGES, LAYERS) + acc_part.shape[1:]) for acc_part in grad_accs]
    y_out = y_rows.reshape(MICROBATCHES, REPLICAS * BATCH_DEV, SEQ_LEN, D_MODEL)
    return (dw_list[0], dw_list[1], dw_list[2], dw_list[3], y_out)
```

```python
import functools

import jax
import jax.numpy as jnp
from jax import lax
from jax.experimental import pallas as pl
from jax.experimental.pallas import tpu as pltpu
from jax.sharding import PartitionSpec as P

HEAD_DIM = 64
PAIR = 2 * HEAD_DIM
NORM_EPS = 1e-6
ROWS_FWD = 2
ROWS_BWD = 2
EXP_SCALE = HEAD_DIM ** -0.5 * 1.4426950408889634
F32 = jnp.float32
BF16 = jnp.bfloat16
NEG = -1e30


def rms_norm(hidden):
    wide_h = hidden.astype(F32)
    return wide_h * lax.rsqrt(jnp.mean(wide_h * wide_h, axis=-1, keepdims=True) + NORM_EPS)


def gelu_tanh(pre_act):
    return jax.nn.gelu(pre_act, approximate=True)


def dot_nn(a, b):
    return lax.dot_general(a, b, (((1,), (0,)), ((), ())), preferred_element_type=F32)


def dot_nt(a, b):
    return lax.dot_general(a, b, (((1,), (1,)), ((), ())), preferred_element_type=F32)


def dot_tn(a, b):
    return lax.dot_general(a, b, (((0,), (0,)), ((), ())), preferred_element_type=F32)


def block_diag(pair, low):
    zero = jnp.zeros_like(pair)
    return jnp.concatenate([jnp.where(low, pair, zero), jnp.where(low, zero, pair)], axis=0)


def attn_fwd_kernel(qkv_ref, out_ref):
    rows, seq, width = qkv_ref.shape
    d_model = width // 3
    low = lax.broadcasted_iota(jnp.int32, (seq, PAIR), 1) < HEAD_DIM
    causal = lax.broadcasted_iota(jnp.int32, (seq, seq), 0) >= lax.broadcasted_iota(jnp.int32, (seq, seq), 1)
    for row in range(rows):
        for col in range(0, d_model, PAIR):
            q = qkv_ref[row, :, col:col + PAIR]
            k = block_diag(qkv_ref[row, :, d_model + col:d_model + col + PAIR], low)
            v = block_diag(qkv_ref[row, :, 2 * d_model + col:2 * d_model + col + PAIR], low)
            scores = dot_nt(q, k)
            probs = []
            for half in range(2):
                s = jnp.where(causal, scores[:, half * seq:(half + 1) * seq], NEG)
                e = jnp.exp2((s - jnp.max(s, axis=-1, keepdims=True)) * EXP_SCALE)
                probs.append((e * (1.0 / jnp.sum(e, axis=-1, keepdims=True))).astype(BF16))
            out_ref[row, :, col:col + PAIR] = dot_nn(jnp.concatenate(probs, axis=1), v).astype(BF16)


def attn_bwd_kernel(qkv_ref, do_ref, dqkv_ref):
    rows, seq, width = qkv_ref.shape
    d_model = width // 3
    low = lax.broadcasted_iota(jnp.int32, (seq, PAIR), 1) < HEAD_DIM
    causal = lax.broadcasted_iota(jnp.int32, (seq, seq), 0) <= lax.broadcasted_iota(jnp.int32, (seq, seq), 1)
    for row in range(rows):
        for col in range(0, d_model, PAIR):
            q = block_diag(qkv_ref[row, :, col:col + PAIR], low)
            k = qkv_ref[row, :, d_model + col:d_model + col + PAIR]
            v = qkv_ref[row, :, 2 * d_model + col:2 * d_model + col + PAIR]
            do = block_diag(do_ref[row, :, col:col + PAIR], low)
            scores = dot_nt(k, q)
            dprobs = dot_nt(v, do)
            probs, dscores = [], []
            for half in range(2):
                s = jnp.where(causal, scores[:, half * seq:(half + 1) * seq], NEG)
                e = jnp.exp2((s - jnp.max(s, axis=0, keepdims=True)) * EXP_SCALE)
                p = (e * (1.0 / jnp.sum(e, axis=0, keepdims=True))).astype(BF16)
                wide = p.astype(F32)
                dp = dprobs[:, half * seq:(half + 1) * seq]
                inner = jnp.sum(dp * wide, axis=0, keepdims=True)
                probs.append(p)
                dscores.append((wide * (dp - inner) * HEAD_DIM ** -0.5).astype(BF16))
            ds_wide = jnp.concatenate(dscores, axis=1)
            ds_tall = jnp.concatenate(dscores, axis=0)
            dqkv_ref[row, :, col:col + PAIR] = dot_tn(ds_tall, block_diag(k, low)).astype(BF16)
            dqkv_ref[row, :, d_model + col:d_model + col + PAIR] = dot_nn(ds_wide, q).astype(BF16)
            dqkv_ref[row, :, 2 * d_model + col:2 * d_model + col + PAIR] = dot_nn(jnp.concatenate(probs, axis=1), do).astype(BF16)


def attn_fwd(qkv, seq):
    tokens, width = qkv.shape
    rows = tokens // seq
    d_model = width // 3
    out = pl.pallas_call(
        attn_fwd_kernel,
        grid=(rows // ROWS_FWD,),
        in_specs=[pl.BlockSpec((ROWS_FWD, seq, width), lambda i: (i, 0, 0))],
        out_specs=pl.BlockSpec((ROWS_FWD, seq, d_model), lambda i: (i, 0, 0)),
        out_shape=jax.ShapeDtypeStruct((rows, seq, d_model), BF16),
        cost_estimate=pl.CostEstimate(flops=8 * tokens * seq * d_model, bytes_accessed=2 * tokens * 4 * d_model, transcendentals=0),
        name="attn_fwd",
    )(qkv.reshape(rows, seq, width))
    return out.reshape(tokens, d_model)


def attn_bwd(qkv, dout, seq):
    tokens, width = qkv.shape
    rows = tokens // seq
    d_model = width // 3
    out = pl.pallas_call(
        attn_bwd_kernel,
        grid=(rows // ROWS_BWD,),
        in_specs=[pl.BlockSpec((ROWS_BWD, seq, width), lambda i: (i, 0, 0)), pl.BlockSpec((ROWS_BWD, seq, d_model), lambda i: (i, 0, 0))],
        out_specs=pl.BlockSpec((ROWS_BWD, seq, width), lambda i: (i, 0, 0)),
        out_shape=jax.ShapeDtypeStruct((rows, seq, width), BF16),
        cost_estimate=pl.CostEstimate(flops=20 * tokens * seq * d_model, bytes_accessed=2 * tokens * 7 * d_model, transcendentals=0),
        name="attn_bwd",
    )(qkv.reshape(rows, seq, width), dout.reshape(rows, seq, d_model))
    return out.reshape(tokens, width)


def layer_forward(hidden, w_qkv, w_out, w_up, w_down, seq):
    normed = rms_norm(hidden).astype(BF16)
    qkv = dot_nn(normed, w_qkv).astype(BF16)
    cat = attn_fwd(qkv, seq)
    mid = (hidden.astype(F32) + dot_nn(cat, w_out)).astype(BF16)
    normed_mid = rms_norm(mid).astype(BF16)
    up = dot_nn(normed_mid, w_up).astype(BF16)
    gelu = gelu_tanh(up.astype(F32)).astype(BF16)
    out = (mid.astype(F32) + dot_nn(gelu, w_down)).astype(BF16)
    return out, (hidden, normed, qkv, cat, mid, normed_mid, up, gelu)


def layer_backward(kept, grad_top, w_qkv, w_out, w_up, w_down, seq, reduce_fn):
    hidden, normed, qkv, cat, mid, normed_mid, up, gelu = kept
    dw_down = reduce_fn(dot_tn(gelu, grad_top), 3)
    grad_gelu = dot_nt(grad_top, w_down)
    _, gelu_pull = jax.vjp(gelu_tanh, up.astype(F32))
    grad_up = gelu_pull(grad_gelu)[0].astype(BF16)
    dw_up = reduce_fn(dot_tn(normed_mid, grad_up), 2)
    grad_nmid = dot_nt(grad_up, w_up)
    _, norm_pull_mid = jax.vjp(rms_norm, mid.astype(F32))
    grad_mid = (grad_top.astype(F32) + norm_pull_mid(grad_nmid)[0]).astype(BF16)
    dw_out = reduce_fn(dot_tn(cat, grad_mid), 1)
    grad_cat = dot_nt(grad_mid, w_out).astype(BF16)
    grad_qkv = attn_bwd(qkv, grad_cat, seq)
    dw_qkv = reduce_fn(dot_tn(normed, grad_qkv), 0)
    grad_normed = dot_nt(grad_qkv, w_qkv)
    _, norm_pull_in = jax.vjp(rms_norm, hidden.astype(F32))
    grad_in = (grad_mid.astype(F32) + norm_pull_in(grad_normed)[0]).astype(BF16)
    return grad_in, (dw_qkv, dw_out, dw_up, dw_down)


def solution(mesh):
    n_stages = mesh.shape["pp"]
    n_rep = mesh.shape["dp"]

    def device_step(x_loc, g_loc, wqkv_loc, wout_loc, wup_loc, wdown_loc):
        n_micro, batch, seq, d_model = x_loc.shape
        stage_idx = lax.axis_index("pp")
        rep_idx = lax.axis_index("dp")
        is_first = stage_idx == 0
        share = n_micro // n_stages
        tokens = share * batch * seq

        def my_half(full):
            return lax.dynamic_slice_in_dim(full, stage_idx * share, share, 0).reshape(tokens, d_model)

        def gather_weight(w_loc):
            rows, cols = w_loc.shape[2:]
            piece = rows // n_rep
            mine = lax.dynamic_slice_in_dim(w_loc.reshape(rows, cols), rep_idx * piece, piece, 0)
            full = lax.all_gather(mine, ("pp", "dp"), axis=0, tiled=True)
            return [full[l * rows:(l + 1) * rows] for l in range(n_stages)]

        weights = list(zip(*[gather_weight(w) for w in (wqkv_loc, wout_loc, wup_loc, wdown_loc)]))

        def reduce_fn(dw, slot):
            return lax.psum_scatter(dw, "dp", scatter_dimension=0, tiled=True)

        hidden = my_half(x_loc)
        kept = []
        for l in range(n_stages):
            hidden, acts = layer_forward(hidden, *weights[l], seq)
            kept.append(acts)
        y_mine = hidden.reshape(share, batch, seq, d_model)
        y_peer = lax.ppermute(y_mine, "pp", [(0, 1), (1, 0)])
        y_full = jnp.where(is_first, jnp.concatenate([y_mine, y_peer]), jnp.concatenate([y_peer, y_mine]))

        grad = my_half(g_loc)
        shards = [None] * n_stages
        for l in reversed(range(n_stages)):
            grad, shards[l] = layer_backward(kept[l], grad, *weights[l], seq, reduce_fn)
        outs = []
        for slot in range(4):
            part = [shards[l][slot] for l in range(n_stages)]
            recv_1 = lax.ppermute(part[1], "pp", [(0, 1)])
            recv_0 = lax.ppermute(part[0], "pp", [(1, 0)])
            outs.append(jnp.where(is_first, part[0] + recv_0, part[1] + recv_1)[None, None])
        return tuple(outs) + (y_full,)

    stage_spec = P("pp")
    shard_spec = P("pp", None, "dp", None)
    return jax.shard_map(device_step, mesh=mesh, in_specs=(P(None, "dp"), P(None, "dp"), stage_spec, stage_spec, stage_spec, stage_spec), out_specs=(shard_spec, shard_spec, shard_spec, shard_spec, P(None, "dp")), check_vma=False)
```
